32 devices in a mesh: row: 8 (over z, x), col: 4 (over y, core).
Axes of the slice: x: 2, y: 2, z: 4, core: 2. Of those that a mesh axis runs over, the one named last changes fastest.
Arguments:
- lower: bfloat16 [8, 3, 512, 2, 512], P('row', None, None, None, 'col'), as said below
- rhs: bfloat16 [8, 3, 512, 8192], P('row', None, None, 'col'), may hold values from -6 to 6
- tile_map: int32 [16], replicated, may hold values from 0 to 15, each once
Outputs:
- overwritten: bfloat16 [8, 3, 512, 8192], P('row', None, None, 'col')
The draws below stay inside these ranges and needn't reach their ends.
Inputs may be any that keep to these rules, and one draw needn't show every extreme that they name: tile_map is a permutation of 0 to 15. lower[0, 0, :, 0, :] and lower[1, 0, :, 1, :] are lower triangular with diagonal entries between 2 and 3; lower[0, 0, :, 1, :] is zero.
All inputs are finite; a program needn't handle non-finite values.
Results may differ from the reference program's by a relative error of at most 0.0032.
Values may be sent and summed in bfloat16 or wider, within the bound.
A program may use at most 128 MiB of HBM per device.

```python
import jax
import jax.numpy as jnp

TB = 512
R = 8192
MT = 3
RT = 16
N_ROW = 8


def draw_lower(key, part):
    keys = jax.random.split(jax.random.fold_in(key, 11), 6)
    shape = (N_ROW, MT, TB, 2, TB)
    base = jax.random.normal(keys[0], shape, jnp.float32)
    base = base * TB ** (-0.5)
    for panel in range(2):
        strict = jax.random.normal(keys[1 + panel], (TB, TB), jnp.float32)
        strict = jnp.tril(strict * 0.8 * TB ** (-0.5), -1)
        values = jax.random.uniform(keys[3 + panel], (TB,), jnp.float32, 2.0, 3.0)
        base = base.at[panel, 0, :, panel, :].set(strict + jnp.diag(values))
    base = base.at[0, 0, :, 1, :].set(0.0)
    return base.astype(jnp.bfloat16)


def block_levels(rng, shape, cuts, smallest, top_value):
    def one(dim, blocks):
        draws = jax.random.uniform(jax.random.fold_in(jax.random.fold_in(rng, 6), dim), (blocks,), jnp.float32, smallest / len(cuts), top_value / len(cuts))
        return jnp.repeat(jnp.exp(draws), shape[dim] // blocks).reshape((-1,) + (1,) * (len(shape) - dim - 1))

    level = one(*cuts[0])
    for cut in cuts[1:]:
        level = level * one(*cut)
    return level


def noise(rng, extent, spread, most, cuts=(), kind=jnp.bfloat16):
    drawn = spread * jax.random.normal(rng, extent, jnp.float32)
    if cuts:
        drawn = drawn * block_levels(rng, extent, cuts, -0.22, 0.18)
    return jnp.clip(drawn, -most, most).astype(kind)


def setup_inputs(seed: int = 0) -> dict:
    arg_keys = jax.random.split(jax.random.key(seed), 4)
    lower = draw_lower(jax.random.fold_in(arg_keys[3], 71), 0)
    rhs = noise(arg_keys[1], (N_ROW, MT, TB, R), 1.0, 6.0, ((0, 8), (3, 4)))
    tile_map = jax.random.permutation(arg_keys[2], RT).astype(jnp.int32)
    return {"lower": lower, "rhs": rhs, "tile_map": tile_map}


def redistribute(array, tile_map):
    shape = array.shape
    tiles = array.reshape(shape[:-1] + (RT, TB))
    return jnp.take(tiles, tile_map, axis=3).reshape(shape)

def reference(lower, rhs, tile_map):
    work = rhs.astype(jnp.float32)
    solved_rows = []
    for panel in range(2):
        diagonal = jnp.tril(lower[panel, 0, :, panel, :].astype(jnp.float32))
        solved = jax.scipy.linalg.solve_triangular(diagonal, work[panel, 0], lower=True).astype(jnp.bfloat16)
        flat = lower[:, :, :, panel, :].reshape(N_ROW * MT * TB, TB)
        update = jnp.dot(flat.astype(jnp.float32), solved.astype(jnp.float32), preferred_element_type=jnp.float32)
        work = work - update.reshape(work.shape)
        solved_rows.append(solved)
    result = work.astype(jnp.bfloat16)
    result = result.at[0, 0].set(solved_rows[0])
    result = result.at[1, 0].set(solved_rows[1])
    return redistribute(result, tile_map)
```

```python
import functools

import jax
import jax.numpy as jnp
from jax import lax
from jax.experimental import pallas as pl
from jax.experimental.pallas import tpu as pltpu
from jax.sharding import PartitionSpec as P

F32 = jnp.float32
BF16 = jnp.bfloat16
ANY = pl.BlockSpec(memory_space=pl.ANY)
VMEM_LIMIT = 56 * 1024 * 1024
CHUNKS = 16
BLOCK = 128


def signal(sem, **where):
    pl.semaphore_signal(sem, inc=1, device_id=where, device_id_type=pl.DeviceIdType.MESH)


def remote(src, dst, send, recv, **where):
    return pltpu.make_async_remote_copy(
        src_ref=src,
        dst_ref=dst,
        send_sem=send,
        recv_sem=recv,
        device_id=where,
        device_id_type=pl.DeviceIdType.MESH,
    )


def spread_kernel(n, rhs, mid, bounce, send, recv, local):
    me = lax.axis_index("col")
    layers, tile, width = rhs.shape
    part = tile // n
    barrier = pltpu.get_barrier_semaphore()
    for d in range(1, n):
        signal(barrier, col=lax.rem(me + d, n))
    pl.semaphore_wait(barrier, n - 1)

    def copy(m, d):
        to = lax.rem(me + d, n)
        return remote(
            rhs.at[m, pl.ds(to * part, part)],
            mid.at[m, :, pl.ds(me * width, width)],
            send.at[m, d - 1],
            recv.at[m, d - 1],
            col=to,
        )

    for m in range(layers):
        for d in range(1, n):
            copy(m, d).start()
    first = pltpu.make_async_copy(rhs.at[:, pl.ds(me * part, part)], bounce, local.at[0])
    first.start()
    first.wait()
    second = pltpu.make_async_copy(bounce, mid.at[:, :, pl.ds(me * width, width)], local.at[1])
    second.start()
    second.wait()
    for m in range(layers):
        for d in range(1, n):
            copy(m, d).wait_recv()
    for m in range(layers):
        for d in range(1, n):
            copy(m, d).wait_send()


def spread(n, rhs):
    layers, tile, width = rhs.shape
    part = tile // n
    return pl.pallas_call(
        functools.partial(spread_kernel, n),
        out_shape=jax.ShapeDtypeStruct((layers, part, width * n), rhs.dtype),
        in_specs=[ANY],
        out_specs=ANY,
        scratch_shapes=[
            pltpu.VMEM((layers, part, width), rhs.dtype),
            pltpu.SemaphoreType.DMA((layers, n - 1)),
            pltpu.SemaphoreType.DMA((layers, n - 1)),
            pltpu.SemaphoreType.DMA((2,)),
        ],
        compiler_params=pltpu.CompilerParams(collective_id=0, has_side_effects=True),
        name="spread",
    )(rhs)


def permute_kernel(order, src, dst):
    dst[...] = src[...]


def permute(mid, tile_map, tile):
    layers, part, width = mid.shape
    return pl.pallas_call(
        permute_kernel,
        out_shape=jax.ShapeDtypeStruct(mid.shape, mid.dtype),
        grid_spec=pltpu.PrefetchScalarGridSpec(
            num_scalar_prefetch=1,
            grid=(width // tile,),
            in_specs=[pl.BlockSpec((layers, part, tile), lambda j, order: (0, 0, order[j]))],
            out_specs=pl.BlockSpec((layers, part, tile), lambda j, order: (0, 0, j)),
        ),
        name="permute",
    )(tile_map, mid)


def collect_kernel(n, n_row, nx, mid, out, cast, bounce, hold, send, recv, zsend, xsend, crecv, local):
    me = lax.axis_index("col")
    row = lax.axis_index("row")
    nz = n_row // nx
    z, x = row // nx, lax.rem(row, nx)
    layers, tile, width = out.shape
    part = tile // n
    step = tile // CHUNKS
    barrier = pltpu.get_barrier_semaphore()
    for d in range(1, n):
        signal(barrier, col=lax.rem(me + d, n))
    for d in range(1, nx):
        signal(barrier, row=z * nx + lax.rem(x + d, nx))
    for d in (1, nz - 1):
        signal(barrier, row=lax.rem(z + d, nz) * nx + x)
    pl.semaphore_wait(barrier, n + nx)

    def copy(m, d):
        to = lax.rem(me + d, n)
        return remote(
            mid.at[m, :, pl.ds(to * width, width)],
            out.at[m, pl.ds(me * part, part)],
            send.at[m, d - 1],
            recv.at[m, d - 1],
            col=to,
        )

    for m in range(layers):
        for d in range(1, n):
            copy(m, d).start()
    first = pltpu.make_async_copy(mid.at[:, :, pl.ds(me * width, width)], bounce, local.at[0])
    first.start()
    first.wait()
    second = pltpu.make_async_copy(bounce, out.at[:, pl.ds(me * part, part)], local.at[1])
    second.start()
    second.wait()
    for d in range(1, n):
        copy(0, d).wait_recv()

    @pl.when(row < 2)
    def _():
        load = pltpu.make_async_copy(out.at[0], hold, local.at[2])
        load.start()
        load.wait()
        store = pltpu.make_async_copy(hold, cast.at[row], local.at[3])
        store.start()
        store.wait()

    def down(k, c):
        piece = cast.at[k, pl.ds(c * step, step)]
        return remote(
            piece, piece, zsend.at[c], crecv.at[k, c], row=lax.rem(z + 1, nz) * nx + x
        )

    def across(k, c, d):
        piece = cast.at[k, pl.ds(c * step, step)]
        return remote(
            piece, piece, xsend.at[c, d - 1], crecv.at[k, c], row=z * nx + lax.rem(x + d, nx)
        )

    for k in range(2):

        @pl.when(x == k)
        def _(k=k):
            @pl.loop(0, CHUNKS)
            def _(c):
                @pl.when(z > 0)
                def _():
                    down(k, c).wait_recv()

                @pl.when(z < nz - 1)
                def _():
                    down(k, c).start()

                for d in range(1, nx):
                    across(k, c, d).start()

    for k in range(2):

        @pl.when(x != k)
        def _(k=k):
            @pl.loop(0, CHUNKS)
            def _(c):
                down(k, c).wait_recv()

        @pl.when(x == k)
        def _(k=k):
            @pl.loop(0, CHUNKS)
            def _(c):
                @pl.when(z < nz - 1)
                def _():
                    down(k, c).wait_send()

                for d in range(1, nx):
                    across(k, c, d).wait_send()

    for m in range(1, layers):
        for d in range(1, n):
            copy(m, d).wait_recv()
    for m in range(layers):
        for d in range(1, n):
            copy(m, d).wait_send()


def collect(n, n_row, mid, tile):
    layers, part, total = mid.shape
    width = total // n
    nx = 2
    while nx * nx * 4 <= n_row:
        nx *= 2
    return pl.pallas_call(
        functools.partial(collect_kernel, n, n_row, nx),
        out_shape=(
            jax.ShapeDtypeStruct((layers, tile, width), mid.dtype),
            jax.ShapeDtypeStruct((2, tile, width), mid.dtype),
        ),
        in_specs=[ANY],
        out_specs=(ANY, ANY),
        scratch_shapes=[
            pltpu.VMEM((layers, part, width), mid.dtype),
            pltpu.VMEM((tile, width), mid.dtype),
            pltpu.SemaphoreType.DMA((layers, n - 1)),
            pltpu.SemaphoreType.DMA((layers, n - 1)),
            pltpu.SemaphoreType.DMA((CHUNKS,)),
            pltpu.SemaphoreType.DMA((CHUNKS, nx - 1)),
            pltpu.SemaphoreType.DMA((2, CHUNKS)),
            pltpu.SemaphoreType.DMA((4,)),
        ],
        compiler_params=pltpu.CompilerParams(collective_id=1, has_side_effects=True),
        name="collect",
    )(mid)


def exact(a, b):
    return jnp.dot(a, b, preferred_element_type=F32, precision=lax.Precision.HIGHEST)


def invert_kernel(blocks, inverse):
    count, size, _ = blocks.shape
    r = lax.broadcasted_iota(jnp.int32, (size, size), 0)
    c = lax.broadcasted_iota(jnp.int32, (size, size), 1)
    lows = [blocks[i].astype(F32) for i in range(count)]
    found = []
    for low in lows:
        found.append(jnp.where(r == c, 1.0 / jnp.where(r == c, low, 1.0), 0.0))
    half = 1
    while half < size:
        keep = (r // (2 * half) == c // (2 * half)) & (r // half > c // half)
        left = [exact(f, jnp.where(keep, low, 0.0)) for f, low in zip(found, lows)]
        found = [f - exact(p, f) for f, p in zip(found, left)]
        half *= 2
    for i in range(count):
        inverse[i] = found[i]


def invert(blocks):
    return pl.pallas_call(
        invert_kernel, out_shape=jax.ShapeDtypeStruct(blocks.shape, F32), name="invert"
    )(blocks)


def apply(low, value):
    high = value.astype(BF16)
    rest = value - high.astype(F32)
    middle = rest.astype(BF16)
    last = (rest - middle.astype(F32)).astype(BF16)
    dot = functools.partial(jnp.dot, preferred_element_type=F32)
    return dot(low, high) + (dot(low, middle) + dot(low, last))


def substitute(low, inverse, first, right):
    tile = low.shape[0]
    found = []
    for i in range(tile // BLOCK):
        rows = slice(i * BLOCK, (i + 1) * BLOCK)
        value = right[rows]
        for j in range(i):
            value = value - apply(low[rows, j * BLOCK : (j + 1) * BLOCK], found[j])
        found.append(exact(inverse[first + i], value))
    return jnp.concatenate(found, axis=0).astype(BF16)


def solve_kernel(place, diag, inverse, panels, cast, rhs, out, both):
    tile = diag.shape[1]
    here = place[0]
    top = substitute(diag.at[0], inverse, 0, cast[0].astype(F32))
    both[:tile] = top
    right = cast[1].astype(F32) - jnp.dot(diag[1], top, preferred_element_type=F32)
    both[tile:] = substitute(diag.at[2], inverse, tile // BLOCK, right)
    for m in range(rhs.shape[0]):
        update = jnp.dot(panels[m], both[...], preferred_element_type=F32)
        out[m] = (rhs[m].astype(F32) - update).astype(BF16)

    @pl.when(here == 0)
    def _():
        out[0] = both[:tile]

    @pl.when(here == 1)
    def _():
        out[0] = both[tile:]


def solve(here, diag, inverse, panels, cast, rhs):
    layers, tile, width = rhs.shape
    wide = min(512, width)

    def whole(shape):
        return pl.BlockSpec(shape, lambda j, place: (0,) * len(shape))

    return pl.pallas_call(
        solve_kernel,
        out_shape=jax.ShapeDtypeStruct(rhs.shape, BF16),
        grid_spec=pltpu.PrefetchScalarGridSpec(
            num_scalar_prefetch=1,
            grid=(width // wide,),
            in_specs=[
                whole(diag.shape),
                whole(inverse.shape),
                whole(panels.shape),
                pl.BlockSpec((2, tile, wide), lambda j, place: (0, 0, j)),
                pl.BlockSpec((layers, tile, wide), lambda j, place: (0, 0, j)),
            ],
            out_specs=pl.BlockSpec((layers, tile, wide), lambda j, place: (0, 0, j)),
            scratch_shapes=[pltpu.VMEM((2 * tile, wide), BF16)],
        ),
        compiler_params=pltpu.CompilerParams(vmem_limit_bytes=VMEM_LIMIT),
        name="solve",
    )(here, diag, inverse, panels, cast, rhs)


def body(n, n_row, lower, rhs, tile_map):
    tile = lower.shape[2]
    here = lax.axis_index("row")
    mine = lower[0]
    roots = jnp.stack(
        [
            jnp.where(here == 0, mine[0, :, 0], 0),
            jnp.where(here == 1, mine[0, :, 0], 0),
            jnp.where(here == 1, mine[0, :, 1], 0),
        ]
    ).astype(BF16)
    roots = lax.psum(roots, "row")
    diag = lax.all_gather(roots, "col", axis=2, tiled=True)
    layers = mine.shape[0]
    panels = lax.all_gather(mine, "col", axis=3, tiled=True).reshape(layers, tile, 2 * tile)
    count = tile // BLOCK
    blocks = jnp.stack(
        [
            jnp.tril(diag[k, i * BLOCK : (i + 1) * BLOCK, i * BLOCK : (i + 1) * BLOCK])
            for k in (0, 2)
            for i in range(count)
        ]
    )
    inverse = invert(blocks)
    mid = permute(spread(n, rhs[0]), tile_map, tile)
    moved, cast = collect(n, n_row, mid, tile)
    place = jnp.reshape(here, (1,)).astype(jnp.int32)
    return solve(place, diag, inverse, panels, cast, moved)[None]


def solution(mesh):
    placed = (P("row", None, None, None, "col"), P("row", None, None, "col"), P())
    return jax.shard_map(
        functools.partial(body, mesh.shape["col"], mesh.shape["row"]),
        mesh=mesh,
        in_specs=placed,
        out_specs=P("row", None, None, "col"),
        check_vma=False,
    )
```

```python
import functools

import jax
import jax.numpy as jnp
from jax import lax
from jax.experimental import pallas as pl
from jax.experimental.pallas import tpu as pltpu
from jax.sharding import PartitionSpec as P

F32 = jnp.float32
BF16 = jnp.bfloat16
ANY = pl.BlockSpec(memory_space=pl.ANY)
VMEM_LIMIT = 56 * 1024 * 1024
CHUNKS = 16
BLOCK = 128


def signal(sem, **where):
    pl.semaphore_signal(sem, inc=1, device_id=where, device_id_type=pl.DeviceIdType.MESH)


def remote(src, dst, send, recv, **where):
    return pltpu.make_async_remote_copy(
        src_ref=src,
        dst_ref=dst,
        send_sem=send,
        recv_sem=recv,
        device_id=where,
        device_id_type=pl.DeviceIdType.MESH,
    )


def spread_kernel(n, n_row, rhs, mine, mid, panels, diag, bounce, hold, send, recv, psend, precv, dsend, drecv, rsend, rrecv, local):
    me = lax.axis_index("col")
    row = lax.axis_index("row")
    chips = n // 2
    chip, core = me // 2, lax.rem(me, 2)
    twin = me + 1 - 2 * core
    layers, tile, width = rhs.shape
    part = tile // n
    barrier = pltpu.get_barrier_semaphore()
    for d in range(1, n):
        signal(barrier, col=lax.rem(me + d, n))

    @pl.loop(1, n_row)
    def _(d):
        signal(barrier, row=lax.rem(row + d, n_row))

    pl.semaphore_wait(barrier, n + n_row - 2)

    def root(slot, d):
        return remote(
            mine.at[0, slot // 2],
            diag.at[me, slot],
            rsend.at[slot, d - 1],
            rrecv.at[slot],
            row=lax.rem(row + d, n_row),
        )

    def from_root(slots, act):
        @pl.loop(1, n_row)
        def _(d):
            for slot in slots:
                act(root(slot, d))

    roots = ((0, (0,)), (1, (1, 2)))
    for owner, slots in roots:

        @pl.when(row == owner)
        def _(slots=slots):
            from_root(slots, lambda c: c.start())

    def over(q):
        return lax.rem(chip + q, chips) * 2 + core

    def cross(source, target, ssem, rsem, q):
        return remote(source, target.at[me], ssem.at[q], rsem.at[q], col=over(q))

    def share(source, target, ssem, rsem, q):
        held = lax.rem(chip + chips - q, chips) * 2 + core
        return remote(
            source if q == 0 else target.at[held],
            target.at[held],
            ssem.at[chips + q],
            rsem.at[chips + q],
            col=twin,
        )

    def copy(m, d):
        to = lax.rem(me + d, n)
        return remote(
            rhs.at[m, pl.ds(to * part, part)],
            mid.at[m, :, pl.ds(me * width, width)],
            send.at[m, d - 1],
            recv.at[m, d - 1],
            col=to,
        )

    for q in range(1, chips):
        cross(mine, panels, psend, precv, q).start()
    share(mine, panels, psend, precv, 0).start()
    for m in range(layers):
        for d in range(1, n):
            copy(m, d).start()
    first = pltpu.make_async_copy(rhs.at[:, pl.ds(me * part, part)], bounce, local.at[0])
    first.start()
    other = pltpu.make_async_copy(mine, hold, local.at[2])
    other.start()
    first.wait()
    second = pltpu.make_async_copy(bounce, mid.at[:, :, pl.ds(me * width, width)], local.at[1])
    second.start()
    other.wait()
    keep = pltpu.make_async_copy(hold, panels.at[me], local.at[3])
    keep.start()
    for owner, slots in roots:

        @pl.when(row == owner)
        def _(slots=slots):
            for slot in slots:
                move = pltpu.make_async_copy(
                    hold.at[0, slot // 2], diag.at[me, slot], local.at[4 + slot]
                )
                move.start()
                move.wait()

        @pl.when(row != owner)
        def _(slots=slots):
            for slot in slots:
                root(slot, 1).wait_recv()

    second.wait()
    keep.wait()
    for q in range(1, chips):
        cross(diag.at[me], diag, dsend, drecv, q).start()
    share(diag.at[me], diag, dsend, drecv, 0).start()
    for source, target, ssem, rsem in ((mine, panels, psend, precv), (diag.at[me], diag, dsend, drecv)):
        for q in range(1, chips):
            cross(source, target, ssem, rsem, q).wait_recv()
            share(source, target, ssem, rsem, q).start()
    for m in range(layers):
        for d in range(1, n):
            copy(m, d).wait_recv()
    for source, target, ssem, rsem in ((mine, panels, psend, precv), (diag.at[me], diag, dsend, drecv)):
        for q in range(chips):
            share(source, target, ssem, rsem, q).wait_recv()
            share(source, target, ssem, rsem, q).wait_send()
        for q in range(1, chips):
            cross(source, target, ssem, rsem, q).wait_send()
    for m in range(layers):
        for d in range(1, n):
            copy(m, d).wait_send()
    for owner, slots in roots:

        @pl.when(row == owner)
        def _(slots=slots):
            from_root(slots, lambda c: c.wait_send())


def spread(n, n_row, rhs, mine):
    layers, tile, width = rhs.shape
    part = tile // n
    deep = mine.shape[-1]
    dma = pltpu.SemaphoreType.DMA
    return pl.pallas_call(
        functools.partial(spread_kernel, n, n_row),
        out_shape=(
            jax.ShapeDtypeStruct((layers, part, width * n), rhs.dtype),
            jax.ShapeDtypeStruct((n,) + mine.shape, mine.dtype),
            jax.ShapeDtypeStruct((n, 3, tile, deep), mine.dtype),
        ),
        in_specs=[ANY, ANY],
        out_specs=(ANY, ANY, ANY),
        scratch_shapes=[
            pltpu.VMEM((layers, part, width), rhs.dtype),
            pltpu.VMEM(mine.shape, mine.dtype),
            dma((layers, n - 1)),
            dma((layers, n - 1)),
            dma((n,)),
            dma((n,)),
            dma((n,)),
            dma((n,)),
            dma((3, n_row - 1)),
            dma((3,)),
            dma((7,)),
        ],
        compiler_params=pltpu.CompilerParams(collective_id=0, has_side_effects=True),
        name="spread",
    )(rhs, mine)


def permute_kernel(tile, order, src, dst, held, load, store):
    count = order.shape[0]

    def fetch(j):
        start = pl.multiple_of(order[j] * tile, tile)
        return pltpu.make_async_copy(src.at[:, :, pl.ds(start, tile)], held.at[j], load.at[j])

    def put(j):
        return pltpu.make_async_copy(held.at[j], dst.at[:, :, pl.ds(j * tile, tile)], store.at[j])

    for j in range(count):
        fetch(j).start()
    for j in range(count):
        fetch(j).wait()
        put(j).start()
    for j in range(count):
        put(j).wait()


def permute(mid, tile_map, tile):
    layers, part, width = mid.shape
    count = width // tile
    return pl.pallas_call(
        functools.partial(permute_kernel, tile),
        out_shape=jax.ShapeDtypeStruct(mid.shape, mid.dtype),
        in_specs=[pl.BlockSpec(memory_space=pltpu.SMEM), ANY],
        out_specs=ANY,
        scratch_shapes=[
            pltpu.VMEM((count, layers, part, tile), mid.dtype),
            pltpu.SemaphoreType.DMA((count,)),
            pltpu.SemaphoreType.DMA((count,)),
        ],
        name="permute",
    )(tile_map, mid)


def collect_kernel(n, n_row, nx, mid, out, cast, bounce, hold, send, recv, zsend, xsend, crecv, local):
    me = lax.axis_index("col")
    row = lax.axis_index("row")
    nz = n_row // nx
    z, x = row // nx, lax.rem(row, nx)
    layers, tile, width = out.shape
    part = tile // n
    step = tile // CHUNKS
    barrier = pltpu.get_barrier_semaphore()
    for d in range(1, n):
        signal(barrier, col=lax.rem(me + d, n))
    for d in range(1, nx):
        signal(barrier, row=z * nx + lax.rem(x + d, nx))
    for d in (1, nz - 1):
        signal(barrier, row=lax.rem(z + d, nz) * nx + x)
    pl.semaphore_wait(barrier, n + nx)

    def copy(m, d):
        to = lax.rem(me + d, n)
        return remote(
            mid.at[m, :, pl.ds(to * width, width)],
            out.at[m, pl.ds(me * part, part)],
            send.at[m, d - 1],
            recv.at[m, d - 1],
            col=to,
        )

    for m in range(layers):
        for d in range(1, n):
            copy(m, d).start()
    first = pltpu.make_async_copy(mid.at[:, :, pl.ds(me * width, width)], bounce, local.at[0])
    first.start()
    first.wait()
    second = pltpu.make_async_copy(bounce, out.at[:, pl.ds(me * part, part)], local.at[1])
    second.start()
    second.wait()
    for d in range(1, n):
        copy(0, d).wait_recv()

    @pl.when(row < 2)
    def _():
        load = pltpu.make_async_copy(out.at[0], hold, local.at[2])
        load.start()
        load.wait()
        store = pltpu.make_async_copy(hold, cast.at[row], local.at[3])
        store.start()
        store.wait()

    def down(k, c):
        piece = cast.at[k, pl.ds(c * step, step)]
        return remote(
            piece, piece, zsend.at[c], crecv.at[k, c], row=lax.rem(z + 1, nz) * nx + x
        )

    def across(k, c, d):
        piece = cast.at[k, pl.ds(c * step, step)]
        return remote(
            piece, piece, xsend.at[c, d - 1], crecv.at[k, c], row=z * nx + lax.rem(x + d, nx)
        )

    for k in range(2):

        @pl.when(x == k)
        def _(k=k):
            @pl.loop(0, CHUNKS)
            def _(c):
                @pl.when(z > 0)
                def _():
                    down(k, c).wait_recv()

                @pl.when(z < nz - 1)
                def _():
                    down(k, c).start()

                for d in range(1, nx):
                    across(k, c, d).start()

    for k in range(2):

        @pl.when(x != k)
        def _(k=k):
            @pl.loop(0, CHUNKS)
            def _(c):
                down(k, c).wait_recv()

        @pl.when(x == k)
        def _(k=k):
            @pl.loop(0, CHUNKS)
            def _(c):
                @pl.when(z < nz - 1)
                def _():
                    down(k, c).wait_send()

                for d in range(1, nx):
                    across(k, c, d).wait_send()

    for m in range(1, layers):
        for d in range(1, n):
            copy(m, d).wait_recv()
    for m in range(layers):
        for d in range(1, n):
            copy(m, d).wait_send()


def collect(n, n_row, mid, tile):
    layers, part, total = mid.shape
    width = total // n
    nx = 2
    while nx * nx * 4 <= n_row:
        nx *= 2
    return pl.pallas_call(
        functools.partial(collect_kernel, n, n_row, nx),
        out_shape=(
            jax.ShapeDtypeStruct((layers, tile, width), mid.dtype),
            jax.ShapeDtypeStruct((2, tile, width), mid.dtype),
        ),
        in_specs=[ANY],
        out_specs=(ANY, ANY),
        scratch_shapes=[
            pltpu.VMEM((layers, part, width), mid.dtype),
            pltpu.VMEM((tile, width), mid.dtype),
            pltpu.SemaphoreType.DMA((layers, n - 1)),
            pltpu.SemaphoreType.DMA((layers, n - 1)),
            pltpu.SemaphoreType.DMA((CHUNKS,)),
            pltpu.SemaphoreType.DMA((CHUNKS, nx - 1)),
            pltpu.SemaphoreType.DMA((2, CHUNKS)),
            pltpu.SemaphoreType.DMA((4,)),
        ],
        compiler_params=pltpu.CompilerParams(collective_id=1, has_side_effects=True),
        name="collect",
    )(mid)


def exact(a, b):
    return jnp.dot(a, b, preferred_element_type=F32, precision=lax.Precision.HIGHEST)


def invert(lows):
    size = lows[0].shape[0]
    r = lax.broadcasted_iota(jnp.int32, (size, size), 0)
    c = lax.broadcasted_iota(jnp.int32, (size, size), 1)
    found = [jnp.where(r == c, 1.0 / jnp.where(r == c, low, 1.0), 0.0) for low in lows]
    half = 1
    while half < size:
        keep = (r // (2 * half) == c // (2 * half)) & (r // half > c // half)
        left = [exact(f, jnp.where(keep, low, 0.0)) for f, low in zip(found, lows)]
        found = [f - exact(p, f) for f, p in zip(found, left)]
        half *= 2
    return found


def terms(value):
    high = value.astype(BF16)
    rest = value - high.astype(F32)
    middle = rest.astype(BF16)
    return high, middle, (rest - middle.astype(F32)).astype(BF16)


def substitute(low, inverse, first, right):
    tile = right.shape[0]
    found, pieces = [], []
    for i in range(tile // BLOCK):
        value = right[i * BLOCK : (i + 1) * BLOCK]
        if i:
            left = low[i * BLOCK : (i + 1) * BLOCK, : i * BLOCK]
            for t in range(3):
                known = jnp.concatenate([p[t] for p in pieces], axis=0)
                value = value - jnp.dot(left, known, preferred_element_type=F32)
        value = exact(inverse[first + i], value)
        found.append(value.astype(BF16))
        pieces.append(terms(value))
    return jnp.concatenate(found, axis=0)


def solve_kernel(place, diag, panels, cast, rhs, out, both, full, tiles, inverse):
    n, layers, _, tile, deep = panels.shape
    count = tile // BLOCK
    here = place[0]

    @pl.when(pl.program_id(0) == 0)
    def _():
        for s in range(n):
            for k in range(3):
                tiles[k, :, s * deep : (s + 1) * deep] = diag[s, k]
            for m in range(layers):
                for k in range(2):
                    at = k * tile + s * deep
                    full[m, :, at : at + deep] = panels[s, m, k]
        lows = []
        for k in (0, 2):
            for i in range(count):
                at = slice(i * BLOCK, (i + 1) * BLOCK)
                lows.append(tiles[k, at, at].astype(F32))
        for i, value in enumerate(invert(lows)):
            inverse[i] = value

    top = substitute(tiles.at[0], inverse, 0, cast[0].astype(F32))
    both[:tile] = top
    right = cast[1].astype(F32) - jnp.dot(tiles[1], top, preferred_element_type=F32)
    both[tile:] = substitute(tiles.at[2], inverse, count, right)
    for m in range(layers):
        update = jnp.dot(full[m], both[...], preferred_element_type=F32)
        out[m] = (rhs[m].astype(F32) - update).astype(BF16)

    @pl.when(here == 0)
    def _():
        out[0] = both[:tile]

    @pl.when(here == 1)
    def _():
        out[0] = both[tile:]


def solve(here, diag, panels, cast, rhs):
    layers, tile, width = rhs.shape
    wide = min(512, width)

    def whole(shape):
        return pl.BlockSpec(
            shape, lambda j, place: (0,) * len(shape), pipeline_mode=pl.Buffered(1)
        )

    def columns(count):
        return pl.BlockSpec((count, tile, wide), lambda j, place: (0, 0, j))

    return pl.pallas_call(
        solve_kernel,
        out_shape=jax.ShapeDtypeStruct(rhs.shape, BF16),
        grid_spec=pltpu.PrefetchScalarGridSpec(
            num_scalar_prefetch=1,
            grid=(width // wide,),
            in_specs=[whole(diag.shape), whole(panels.shape), columns(2), columns(layers)],
            out_specs=columns(layers),
            scratch_shapes=[
                pltpu.VMEM((2 * tile, wide), BF16),
                pltpu.VMEM((layers, tile, 2 * tile), BF16),
                pltpu.VMEM((3, tile, tile), BF16),
                pltpu.VMEM((2 * tile // BLOCK, BLOCK, BLOCK), F32),
            ],
        ),
        compiler_params=pltpu.CompilerParams(vmem_limit_bytes=VMEM_LIMIT),
        name="solve",
    )(here, diag, panels, cast, rhs)


def body(n, n_row, lower, rhs, tile_map):
    tile = lower.shape[2]
    here = lax.axis_index("row")
    mine = jnp.transpose(lower[0], (0, 2, 1, 3))
    mid, panels, diag = spread(n, n_row, rhs[0], mine)
    moved, cast = collect(n, n_row, permute(mid, tile_map, tile), tile)
    place = jnp.reshape(here, (1,)).astype(jnp.int32)
    return solve(place, diag, panels, cast, moved)[None]


def solution(mesh):
    placed = (P("row", None, None, None, "col"), P("row", None, None, "col"), P())
    return jax.shard_map(
        functools.partial(body, mesh.shape["col"], mesh.shape["row"]),
        mesh=mesh,
        in_specs=placed,
        out_specs=P("row", None, None, "col"),
        check_vma=False,
    )
```
